32 devices in a mesh: seq: 16 (over z, y, core), mp: 2 (over x).
Axes of the slice: x: 2, y: 2, z: 4, core: 2. Of those that a mesh axis runs over, the one named last changes fastest.
Arguments:
- stream: bfloat16 [2048, 8192], P('seq', 'mp'), may hold values from -17 to 17
- norm_gain: float32 [8192], P('mp'), may hold values from 0.5 to 1.5
- short_outer: bfloat16 [2048, 8192], P('seq', 'mp'), may hold values from -4 to 4
- short_inner: bfloat16 [2048, 8192], P('seq', 'mp'), may hold values from -4 to 4
- short_filter: bfloat16 [128, 8192], P(None, 'mp'), may hold values from -0.5 to 0.5
- long_outer: bfloat16 [2048, 8192], P('seq', 'mp'), may hold values from -4 to 4
- long_inner: bfloat16 [2048, 8192], P('seq', 'mp'), may hold values from -4 to 4
- long_decay: float32 [8192], P('mp'), may hold values from 1e-06 to 0.03
- query_heads: bfloat16 [2048, 8192], P('seq', 'mp'), may hold values from -6 to 6
- key_heads: bfloat16 [2048, 8192], P('seq', 'mp'), may hold values from -6 to 6
Outputs:
- long_mixed: bfloat16 [2048, 8192], P('seq', 'mp')
- attended: bfloat16 [2048, 8192], P('seq', 'mp')
The draws below stay inside these ranges and needn't reach their ends.
All inputs are finite; a program needn't handle non-finite values.
Results may differ from the reference program's by a relative error of at most 0.013.
Values may be sent and summed in bfloat16 or wider, within the bound.
A program may use at most 64 MiB of HBM per device.

```python
import math
import jax
import jax.numpy as jnp
from jax import lax

D = 8192
HEADS = 64
HEAD_DIM = 128
TAPS = 128
TOK_DEV = 128
SEQ_LEN = 2048
N_SEQ = 16


def draw_stream(key, part):
    shape = (SEQ_LEN, D // 128, 128)
    base = jnp.clip(jax.random.normal(jax.random.fold_in(key, 11), shape, jnp.float32), -4.0, 4.0)
    levels = jnp.exp(jax.random.uniform(jax.random.fold_in(key, 13), (SEQ_LEN, D // 128, 1), jnp.float32, -1.4, 1.4))
    return (base * levels).reshape(SEQ_LEN, D).astype(jnp.bfloat16)


def draw_long_decay(key, part):
    upper = math.log(0.03)
    return jnp.exp(jax.random.uniform(jax.random.fold_in(key, 41), (D,), jnp.float32, math.log(1e-06), upper))


def draw_heads(key, salt):
    drawn = jnp.clip(jax.random.normal(jax.random.fold_in(key, salt), (SEQ_LEN, D), jnp.float32), -6.0, 6.0)
    return drawn


def draw_query_heads(key, part):
    return draw_heads(key, 31).astype(jnp.bfloat16)


def draw_key_heads(key, part):
    return draw_heads(key, 32).astype(jnp.bfloat16)


def block_scale(rng, extent, split, low, high):
    loudness, own = 1.0, jax.random.fold_in(rng, 6)
    for axis_at, parts in split:
        heights = jnp.exp(jax.random.uniform(jax.random.fold_in(own, axis_at), (parts,), jnp.float32, low / len(split), high / len(split)))
        loudness = loudness * jnp.repeat(heights, extent[axis_at] // parts).reshape([-1 if axis == axis_at else 1 for axis in range(len(extent))])
    return loudness


def normal_values(key, extent, width, most, cuts=(), kind=jnp.bfloat16):
    values = width * jax.random.normal(key, extent, jnp.float32)
    if cuts:
        values = values * block_scale(key, extent, cuts, -0.22, 0.18)
    return jnp.clip(values, -most, most).astype(kind)


def setup_inputs(seed: int = 0) -> dict:
    key_list = jax.random.split(jax.random.key(seed), 11)
    stream = draw_stream(jax.random.fold_in(key_list[10], 71), 0)
    norm_gain = jnp.clip(1.0 + 0.1 * jax.random.normal(key_list[1], (D,), jnp.float32), 0.5, 1.5)
    short_outer = normal_values(key_list[2], (SEQ_LEN, D), 1.0, 4.0, ((0, 16), (1, 2)))
    short_inner = normal_values(key_list[3], (SEQ_LEN, D), 1.0, 4.0, ((0, 16), (1, 2)))
    short_filter = normal_values(key_list[4], (TAPS, D), TAPS ** -0.5, 0.5, ((1, 2),))
    long_outer = normal_values(key_list[5], (SEQ_LEN, D), 1.0, 4.0, ((0, 16), (1, 2)))
    long_inner = normal_values(key_list[6], (SEQ_LEN, D), 1.0, 4.0, ((0, 16), (1, 2)))
    long_decay = draw_long_decay(jax.random.fold_in(key_list[10], 71), 0)
    query_heads = draw_query_heads(jax.random.fold_in(key_list[10], 71), 0)
    key_heads = draw_key_heads(jax.random.fold_in(key_list[10], 71), 0)
    return {"stream": stream, "norm_gain": norm_gain, "short_outer": short_outer, "short_inner": short_inner, "short_filter": short_filter, "long_outer": long_outer, "long_inner": long_inner, "long_decay": long_decay, "query_heads": query_heads, "key_heads": key_heads}


def pair_combine(first_pair, second_pair):
    return (first_pair[0] * second_pair[0], second_pair[0] * first_pair[1] + second_pair[1])

def reference(stream, norm_gain, short_outer, short_inner, short_filter, long_outer, long_inner, long_decay, query_heads, key_heads):
    rates = jnp.exp(-long_decay)
    scales = jnp.sqrt(-jnp.expm1(-2.0 * long_decay))
    filt = short_filter.astype(jnp.float32)

    def blocked(array):
        return array.reshape(N_SEQ, TOK_DEV, D)
    inputs = (jnp.arange(N_SEQ, dtype=jnp.int32), blocked(stream), blocked(short_outer), blocked(short_inner), blocked(long_outer), blocked(long_inner), blocked(query_heads), blocked(key_heads))

    def block_step(carry, pieces):
        tail, state, prev_keys, prev_values = carry
        block_index, x_blk, s_outer, s_inner, l_outer, l_inner, q_blk, k_blk = pieces
        x_float = x_blk.astype(jnp.float32)
        mean_square = lax.optimization_barrier(jnp.mean(x_float * x_float, axis=1, keepdims=True))
        normed = x_float * norm_gain / jnp.sqrt(mean_square + 0.5)
        short_in = (s_inner.astype(jnp.float32) * normed).astype(jnp.bfloat16)
        extended = jnp.concatenate([tail, short_in], axis=0).astype(jnp.float32)

        def tap_step(j, acc):
            start = (TAPS - 1 - j).astype(jnp.int32)
            window = lax.dynamic_slice_in_dim(extended, start, TOK_DEV, 0)
            return acc + lax.dynamic_slice_in_dim(filt, j.astype(jnp.int32), 1, 0) * window
        short_conv = lax.fori_loop(0, TAPS, tap_step, jnp.zeros((TOK_DEV, D), jnp.float32))
        long_in = (l_inner.astype(jnp.float32) * s_outer.astype(jnp.float32) * short_conv).astype(jnp.bfloat16)
        factors = jnp.broadcast_to(rates, long_in.shape)
        powers, states = lax.associative_scan(pair_combine, (factors, long_in.astype(jnp.float32)), axis=0)
        states = states + powers * state
        long_mixed = (l_outer.astype(jnp.float32) * (states * scales)).astype(jnp.bfloat16)
        query = q_blk.astype(jnp.float32).reshape(TOK_DEV, HEADS, HEAD_DIM)
        keys = jnp.concatenate([prev_keys, k_blk], axis=0).astype(jnp.float32).reshape(2 * TOK_DEV, HEADS, HEAD_DIM)
        values = jnp.concatenate([prev_values, long_mixed], axis=0).astype(jnp.float32).reshape(2 * TOK_DEV, HEADS, HEAD_DIM)
        scores = jnp.einsum('thd,shd->hts', query, keys) * HEAD_DIM ** (-0.5)
        row_pos = jnp.arange(TOK_DEV, dtype=jnp.int32)[:, None]
        col_pos = jnp.arange(2 * TOK_DEV, dtype=jnp.int32)[None, :]
        valid = (col_pos <= row_pos + TOK_DEV) & ((col_pos >= TOK_DEV) | (block_index > 0))
        scores = jnp.where(valid[None], scores, -1e+30)
        weights = jax.nn.softmax(scores, axis=-1).astype(jnp.bfloat16)
        result = jnp.einsum('hts,shd->thd', weights.astype(jnp.float32), values)
        attended = result.reshape(TOK_DEV, D).astype(jnp.bfloat16)
        new_carry = (short_in[TOK_DEV - (TAPS - 1):], states[-1], k_blk, long_mixed)
        return (new_carry, (long_mixed, attended))
    start_carry = (jnp.zeros((TAPS - 1, D), jnp.bfloat16), jnp.zeros((D,), jnp.float32), jnp.zeros((TOK_DEV, D), jnp.bfloat16), jnp.zeros((TOK_DEV, D), jnp.bfloat16))
    _, outputs = lax.scan(block_step, start_carry, inputs)
    long_mixed = outputs[0].reshape(SEQ_LEN, D)
    attended = outputs[1].reshape(SEQ_LEN, D)
    return (long_mixed, attended)
```

```python
import functools

import jax
import jax.numpy as jnp
import numpy as np
from jax import lax
from jax.experimental import pallas as pl
from jax.experimental.pallas import tpu as pltpu
from jax.sharding import PartitionSpec as P

HEAD_DIM = 128
CHUNKS = 4
TILE = 256
MESH = pl.DeviceIdType.MESH


def dft_matrices(rows):
    size = 2 * rows
    theta = 2.0 * np.pi * (np.arange(rows) + 0.5) / size
    angle = theta[:, None] * np.arange(size)[None, :]
    forward = np.concatenate([np.cos(angle), -np.sin(angle)], axis=0)
    late = angle[:, rows:].T
    inverse = np.concatenate([np.cos(late), -np.sin(late)], axis=1) / rows
    return forward, inverse


def dot(a, b):
    return jnp.dot(a, b, preferred_element_type=jnp.float32)


def kernel(
    n,
    mp,
    channels,
    gain_ref,
    decay_ref,
    stream_hbm,
    souter_hbm,
    sinner_hbm,
    filt_hbm,
    louter_hbm,
    linner_hbm,
    query_hbm,
    key_hbm,
    fwd_hbm,
    inv_hbm,
    mixed_hbm,
    attended_hbm,
    stream,
    souter,
    sinner,
    filt,
    louter,
    linner,
    query,
    fwd,
    inv,
    keys,
    values,
    ext,
    power,
    inv_power,
    cum,
    spectrum,
    weights,
    attended,
    squares,
    squares_in,
    own_state,
    states,
    load_sem,
    key_sem,
    store_sem,
    sq_send,
    sq_recv,
    k_send,
    k_recv,
    t_send,
    t_recv,
    v_send,
    v_recv,
    e_send,
    e_recv,
):
    me = lax.axis_index("seq")
    col = lax.axis_index("mp")
    rows, width = stream.shape
    wide = width // CHUNKS
    tiles = wide // TILE
    heads = wide // HEAD_DIM
    has_next = me < n - 1
    has_prev = me > 0
    own = pl.ds(rows, rows)
    before = pl.ds(0, rows)

    barrier = pltpu.get_barrier_semaphore()

    def greet(k, _):
        pl.semaphore_signal(
            barrier, inc=1, device_id={"seq": lax.rem(me + k, n)}, device_id_type=MESH
        )
        return 0

    lax.fori_loop(1, n, greet, 0)
    for k in range(1, mp):
        pl.semaphore_signal(
            barrier, inc=1, device_id={"mp": lax.rem(col + k, mp)}, device_id_type=MESH
        )

    pairs = [
        (stream_hbm, stream),
        (fwd_hbm, fwd),
        (filt_hbm, filt),
        (sinner_hbm, sinner),
        (inv_hbm, inv),
        (souter_hbm, souter),
        (linner_hbm, linner),
        (louter_hbm, louter),
        (query_hbm, query),
    ]
    loads = [pltpu.make_async_copy(s, d, load_sem.at[i]) for i, (s, d) in enumerate(pairs)]
    key_loads = [
        pltpu.make_async_copy(
            key_hbm.at[:, pl.ds(c * wide, wide)], keys.at[c, own], key_sem.at[c]
        )
        for c in range(CHUNKS)
    ]
    loads[0].start()
    key_loads[0].start()
    for copy in loads[1:]:
        copy.start()
    for copy in key_loads[1:]:
        copy.start()

    def to_next(buffer, c, send, recv):
        return pltpu.make_async_remote_copy(
            src_ref=buffer.at[c, own],
            dst_ref=buffer.at[c, before],
            send_sem=send.at[c],
            recv_sem=recv.at[c],
            device_id={"seq": lax.rem(me + 1, n)},
            device_id_type=MESH,
        )

    k_copies = [to_next(keys, c, k_send, k_recv) for c in range(CHUNKS)]
    t_copies = [to_next(ext, c, t_send, t_recv) for c in range(CHUNKS)]
    v_copies = [to_next(values, c, v_send, v_recv) for c in range(CHUNKS)]

    @pl.when(me == 0)
    def _():
        for c in range(CHUNKS):
            keys[c, :rows, :] = jnp.zeros((rows, wide), keys.dtype)
            values[c, :rows, :] = jnp.zeros((rows, wide), values.dtype)
            ext[c, :rows, :] = jnp.zeros((rows, wide), ext.dtype)

    loads[0].wait()

    def square(i, acc):
        x = stream[:, pl.ds(pl.multiple_of(i * 128, 128), 128)].astype(jnp.float32)
        return acc + x * x

    squares[...] = lax.fori_loop(
        0, width // 128, square, jnp.zeros((rows, 128), jnp.float32), unroll=4
    )
    pl.semaphore_wait(barrier, n - 1 + mp - 1)
    sq_copies = [
        pltpu.make_async_remote_copy(
            src_ref=squares,
            dst_ref=squares_in.at[k - 1],
            send_sem=sq_send.at[k - 1],
            recv_sem=sq_recv.at[k - 1],
            device_id={"mp": lax.rem(col + k, mp)},
            device_id_type=MESH,
        )
        for k in range(1, mp)
    ]
    for copy in sq_copies:
        copy.start()
    key_loads[0].wait()

    @pl.when(has_next)
    def _():
        k_copies[0].start()

    for copy in loads[1:4]:
        copy.wait()

    def spectra(i, _):
        cols = pl.ds(pl.multiple_of(i * TILE, TILE), TILE)
        spectrum[:, cols] = dot(fwd[:, :rows], filt[:, cols])
        return 0

    lax.fori_loop(0, width // TILE, spectra, 0)

    total = squares[...]
    for k, copy in enumerate(sq_copies):
        copy.wait_recv()
        total = total + squares_in[k]
    mean_square = jnp.sum(total, axis=1, keepdims=True) / channels
    norm = 1.0 / jnp.sqrt(mean_square + 0.5)

    for c in range(CHUNKS):

        def short(i, _, c=c):
            cols = pl.ds(pl.multiple_of(c * wide + i * TILE, TILE), TILE)
            x = stream[:, cols].astype(jnp.float32) * gain_ref[:, cols] * norm
            ext[c, own, pl.ds(pl.multiple_of(i * TILE, TILE), TILE)] = (
                sinner[:, cols].astype(jnp.float32) * x
            ).astype(jnp.bfloat16)
            return 0

        lax.fori_loop(0, tiles, short, 0)

        @pl.when(has_next)
        def _(c=c):
            t_copies[c].start()

    step = lax.broadcasted_iota(jnp.int32, (rows, TILE), 0).astype(jnp.float32)

    def powers(i, _):
        cols = pl.ds(pl.multiple_of(i * TILE, TILE), TILE)
        exponent = step * decay_ref[:, cols]
        power[:, cols] = jnp.exp(-exponent)
        inv_power[:, cols] = jnp.exp(exponent)
        return 0

    lax.fori_loop(0, width // TILE, powers, 0)
    for copy in loads[4:]:
        copy.wait()
    row = lax.broadcasted_iota(jnp.int32, (rows, 2 * rows), 0)
    column = lax.broadcasted_iota(jnp.int32, (rows, 2 * rows), 1)
    lower = (jnp.where(column >= rows, column - rows, column) <= row).astype(
        jnp.float32
    ).astype(jnp.bfloat16)

    def state_copy(c, target):
        return pltpu.make_async_remote_copy(
            src_ref=own_state.at[c],
            dst_ref=states.at[c, me],
            send_sem=e_send.at[c, target],
            recv_sem=e_recv.at[c, me],
            device_id={"seq": target},
            device_id_type=MESH,
        )

    for c in range(CHUNKS):

        @pl.when(has_prev)
        def _(c=c):
            t_copies[c].wait_recv()

        def mix(i, _, c=c):
            here = pl.ds(pl.multiple_of(i * TILE, TILE), TILE)
            cols = pl.ds(pl.multiple_of(c * wide + i * TILE, TILE), TILE)
            x = dot(fwd[...], ext[c, :, here])
            x_re, x_im = x[:rows], x[rows:]
            h_re, h_im = spectrum[:rows, cols], spectrum[rows:, cols]
            y = jnp.concatenate(
                [x_re * h_re - x_im * h_im, x_re * h_im + x_im * h_re], axis=0
            ).astype(jnp.bfloat16)
            conv = dot(inv[...], y)
            long_in = (
                linner[:, cols].astype(jnp.float32) * souter[:, cols].astype(jnp.float32) * conv
            ).astype(jnp.bfloat16)
            v = long_in.astype(jnp.float32) * inv_power[:, cols]
            high = v.astype(jnp.bfloat16)
            low = (v - high.astype(jnp.float32)).astype(jnp.bfloat16)
            sums = dot(lower, jnp.concatenate([high, low], axis=0))
            cum[:, cols] = sums
            own_state[c, :, here] = sums[rows - 1 :] * power[rows - 1 :, cols]
            return 0

        lax.fori_loop(0, tiles, mix, 0)

        def send_state(target, _, c=c):
            state_copy(c, target).start()
            return 0

        lax.fori_loop(me + 1, n, send_state, 0)

    for copy in key_loads[1:]:
        copy.wait()

    @pl.when(has_next)
    def _():
        for c in range(1, CHUNKS):
            k_copies[c].start()

    mixed_stores = []
    for c in range(CHUNKS):
        chunk = pl.ds(c * wide, wide)
        rate = decay_ref[:, chunk]
        over_block = jnp.exp(-rate * rows)

        def arrive(j, state, c=c, over_block=over_block):
            pltpu.make_async_remote_copy(
                src_ref=own_state.at[c],
                dst_ref=states.at[c, j],
                send_sem=e_send.at[c, me],
                recv_sem=e_recv.at[c, j],
                device_id={"seq": j},
                device_id_type=MESH,
            ).wait_recv()
            return state * over_block + states[c, j]

        carried = lax.fori_loop(0, me, arrive, jnp.zeros((1, wide), jnp.float32))
        carried = carried * jnp.exp(-rate)
        z = 2.0 * rate
        scale = jnp.sqrt(jnp.tanh(0.5 * z) * (1.0 + jnp.exp(-z)))
        for i in range(tiles):
            here = pl.ds(i * TILE, TILE)
            cols = pl.ds(c * wide + i * TILE, TILE)
            part = slice(i * TILE, (i + 1) * TILE)
            conv = (cum[:, cols] + carried[:, part]) * power[:, cols]
            values[c, own, here] = (
                louter[:, cols].astype(jnp.float32) * (conv * scale[:, part])
            ).astype(jnp.bfloat16)

        @pl.when(has_next)
        def _(c=c):
            v_copies[c].start()

        store = pltpu.make_async_copy(
            values.at[c, own], mixed_hbm.at[:, chunk], store_sem.at[c]
        )
        store.start()
        mixed_stores.append(store)

    valid = (column <= row + rows) & ((column >= rows) | has_prev)
    for c in range(CHUNKS):

        @pl.when(has_prev)
        def _(c=c):
            k_copies[c].wait_recv()

        def score(h, _, c=c):
            here = pl.ds(pl.multiple_of(h * HEAD_DIM, HEAD_DIM), HEAD_DIM)
            cols = pl.ds(pl.multiple_of(c * wide + h * HEAD_DIM, HEAD_DIM), HEAD_DIM)
            s = lax.dot_general(
                query[:, cols],
                keys[c, :, here],
                (((1,), (1,)), ((), ())),
                preferred_element_type=jnp.float32,
            ) * HEAD_DIM ** (-0.5)
            s = jnp.where(valid, s, -1e30)
            e = jnp.exp(s - jnp.max(s, axis=1, keepdims=True))
            e = e * (1.0 / jnp.sum(e, axis=1, keepdims=True))
            weights[c, h] = e.astype(jnp.bfloat16)
            return 0

        lax.fori_loop(0, heads, score, 0, unroll=2)

    out_stores = []
    for c in range(CHUNKS):

        @pl.when(has_prev)
        def _(c=c):
            v_copies[c].wait_recv()

        def gather(h, _, c=c):
            here = pl.ds(pl.multiple_of(h * HEAD_DIM, HEAD_DIM), HEAD_DIM)
            attended[c, :, here] = dot(weights[c, h], values[c, :, here]).astype(jnp.bfloat16)
            return 0

        lax.fori_loop(0, heads, gather, 0, unroll=2)
        store = pltpu.make_async_copy(
            attended.at[c], attended_hbm.at[:, pl.ds(c * wide, wide)], store_sem.at[CHUNKS + c]
        )
        store.start()
        out_stores.append(store)

    for copy in sq_copies:
        copy.wait_send()

    for c in range(CHUNKS):

        def sent(target, _, c=c):
            state_copy(c, target).wait_send()
            return 0

        lax.fori_loop(me + 1, n, sent, 0)

    @pl.when(has_next)
    def _():
        for copy in k_copies + t_copies + v_copies:
            copy.wait_send()

    for store in mixed_stores + out_stores:
        store.wait()


def on_device(
    n,
    mp,
    stream,
    norm_gain,
    short_outer,
    short_inner,
    short_filter,
    long_outer,
    long_inner,
    long_decay,
    query_heads,
    key_heads,
):
    rows, width = stream.shape
    wide = width // CHUNKS
    forward, inverse = dft_matrices(rows)
    bf16, f32 = jnp.bfloat16, jnp.float32
    anywhere = pl.BlockSpec(memory_space=pl.ANY)
    vmem = pl.BlockSpec(memory_space=pltpu.VMEM)
    dma = pltpu.SemaphoreType.DMA
    return pl.pallas_call(
        functools.partial(kernel, n, mp, float(width * mp)),
        out_shape=[jax.ShapeDtypeStruct((rows, width), bf16)] * 2,
        in_specs=[vmem] * 2 + [anywhere] * 10,
        out_specs=[anywhere] * 2,
        scratch_shapes=[pltpu.VMEM((rows, width), bf16)] * 7
        + [
            pltpu.VMEM((2 * rows, 2 * rows), bf16),
            pltpu.VMEM((rows, 2 * rows), bf16),
        ]
        + [pltpu.VMEM((CHUNKS, 2 * rows, wide), bf16)] * 3
        + [pltpu.VMEM((rows, width), f32)] * 3
        + [
            pltpu.VMEM((2 * rows, width), f32),
            pltpu.VMEM((CHUNKS, wide // HEAD_DIM, rows, 2 * rows), bf16),
            pltpu.VMEM((CHUNKS, rows, wide), bf16),
            pltpu.VMEM((rows, 128), f32),
            pltpu.VMEM((mp - 1, rows, 128), f32),
            pltpu.VMEM((CHUNKS, 1, wide), f32),
            pltpu.VMEM((CHUNKS, n, 1, wide), f32),
            dma((9,)),
            dma((CHUNKS,)),
            dma((2 * CHUNKS,)),
            dma((mp - 1,)),
            dma((mp - 1,)),
        ]
        + [dma((CHUNKS,))] * 6
        + [dma((CHUNKS, n))] * 2,
        compiler_params=pltpu.CompilerParams(
            collective_id=0, has_side_effects=True, vmem_limit_bytes=60 * 1024 * 1024
        ),
    )(
        norm_gain.reshape(1, width),
        long_decay.reshape(1, width),
        stream,
        short_outer,
        short_inner,
        short_filter,
        long_outer,
        long_inner,
        query_heads,
        key_heads,
        jnp.asarray(forward, bf16),
        jnp.asarray(inverse, bf16),
    )


def solution(mesh):
    return jax.shard_map(
        functools.partial(on_device, mesh.shape["seq"], mesh.shape["mp"]),
        mesh=mesh,
        in_specs=(
            P("seq", "mp"),
            P("mp"),
            P("seq", "mp"),
            P("seq", "mp"),
            P(None, "mp"),
            P("seq", "mp"),
            P("seq", "mp"),
            P("mp"),
            P("seq", "mp"),
            P("seq", "mp"),
        ),
        out_specs=(P("seq", "mp"), P("seq", "mp")),
        check_vma=False,
    )
```

```python
import functools

import jax
import jax.numpy as jnp
import numpy as np
from jax import lax
from jax.experimental import pallas as pl
from jax.experimental.pallas import tpu as pltpu
from jax.sharding import PartitionSpec as P

HEAD_DIM = 128
CHUNKS = 4
PAIR = 2
TILE = 256
MESH = pl.DeviceIdType.MESH


def wave(frequency, place, rows):
    shift = jnp.where(frequency >= rows, rows, 0)
    index = lax.rem((2 * lax.rem(frequency, rows) + 1) * place + shift, 4 * rows)
    return jnp.cos(index.astype(jnp.float32) * (np.pi / (2 * rows)))


def dot(a, b):
    return jnp.dot(a, b, preferred_element_type=jnp.float32)


def kernel(
    n,
    mp,
    channels,
    gain_ref,
    decay_ref,
    stream_hbm,
    souter_hbm,
    sinner_hbm,
    filt_hbm,
    louter_hbm,
    linner_hbm,
    query_hbm,
    key_hbm,
    mixed,
    attended,
    stream,
    souter,
    sinner,
    filt,
    louter,
    linner,
    query,
    fwd,
    inv,
    keys,
    values,
    ext,
    power,
    inv_power,
    cum,
    spectrum,
    weights,
    squares,
    squares_in,
    own_state,
    pair_state,
    group_state,
    next_state,
    carry_in,
    states,
    load_sem,
    key_sem,
    sq_send,
    sq_recv,
    k_send,
    k_recv,
    t_send,
    t_recv,
    v_send,
    v_recv,
    p_send,
    p_recv,
    q_send,
    q_recv,
    e_send,
    e_recv,
):
    me = lax.axis_index("seq")
    col = lax.axis_index("mp")
    rows, width = stream.shape
    wide = width // CHUNKS
    tiles = wide // TILE
    heads = wide // HEAD_DIM
    has_next = me < n - 1
    has_prev = me > 0
    groups = n // PAIR
    group = me // PAIR
    leads = lax.rem(me, PAIR) == 0
    follows = lax.rem(me, PAIR) != 0
    own = pl.ds(rows, rows)
    before = pl.ds(0, rows)

    barrier = pltpu.get_barrier_semaphore()

    def greet(target):
        pl.semaphore_signal(barrier, inc=1, device_id={"seq": target}, device_id_type=MESH)

    @pl.when(has_next)
    def _():
        greet(me + 1)

    @pl.when(has_prev)
    def _():
        greet(me - 1)

    @pl.when(leads)
    def _():
        def greet_leader(k, _):
            greet(lax.rem(me + PAIR * k, n))
            return 0

        lax.fori_loop(1, groups, greet_leader, 0)

    for k in range(1, mp):
        pl.semaphore_signal(
            barrier, inc=1, device_id={"mp": lax.rem(col + k, mp)}, device_id_type=MESH
        )

    pairs = [
        (stream_hbm, stream),
        (filt_hbm, filt),
        (sinner_hbm, sinner),
        (souter_hbm, souter),
        (linner_hbm, linner),
        (louter_hbm, louter),
        (query_hbm, query),
    ]
    loads = [pltpu.make_async_copy(s, d, load_sem.at[i]) for i, (s, d) in enumerate(pairs)]
    key_loads = [
        pltpu.make_async_copy(
            key_hbm.at[:, pl.ds(c * wide, wide)], keys.at[c, own], key_sem.at[c]
        )
        for c in range(CHUNKS)
    ]
    loads[0].start()
    key_loads[0].start()
    for copy in loads[1:]:
        copy.start()
    for copy in key_loads[1:]:
        copy.start()

    def to_next(buffer, c, send, recv):
        return pltpu.make_async_remote_copy(
            src_ref=buffer.at[c, own],
            dst_ref=buffer.at[c, before],
            send_sem=send.at[c],
            recv_sem=recv.at[c],
            device_id={"seq": lax.rem(me + 1, n)},
            device_id_type=MESH,
        )

    k_copies = [to_next(keys, c, k_send, k_recv) for c in range(CHUNKS)]
    t_copies = [to_next(ext, c, t_send, t_recv) for c in range(CHUNKS)]
    v_copies = [to_next(values, c, v_send, v_recv) for c in range(CHUNKS)]

    @pl.when(me == 0)
    def _():
        for c in range(CHUNKS):
            keys[c, :rows, :] = jnp.zeros((rows, wide), keys.dtype)
            values[c, :rows, :] = jnp.zeros((rows, wide), values.dtype)
            ext[c, :rows, :] = jnp.zeros((rows, wide), ext.dtype)

    loads[0].wait()

    def square(i, acc):
        x = stream[:, pl.ds(pl.multiple_of(i * 128, 128), 128)].astype(jnp.float32)
        return acc + x * x

    squares[...] = lax.fori_loop(
        0, width // 128, square, jnp.zeros((rows, 128), jnp.float32), unroll=4
    )
    greeted = has_next.astype(jnp.int32) + has_prev.astype(jnp.int32) + mp - 1
    pl.semaphore_wait(barrier, jnp.where(leads, greeted + groups - 1, greeted))
    sq_copies = [
        pltpu.make_async_remote_copy(
            src_ref=squares,
            dst_ref=squares_in.at[k - 1],
            send_sem=sq_send.at[k - 1],
            recv_sem=sq_recv.at[k - 1],
            device_id={"mp": lax.rem(col + k, mp)},
            device_id_type=MESH,
        )
        for k in range(1, mp)
    ]
    for copy in sq_copies:
        copy.start()
    key_loads[0].wait()

    @pl.when(has_next)
    def _():
        k_copies[0].start()

    for copy in loads[1:3]:
        copy.wait()

    full = (2 * rows, 2 * rows)
    fwd[...] = wave(
        lax.broadcasted_iota(jnp.int32, full, 0), lax.broadcasted_iota(jnp.int32, full, 1), rows
    ).astype(jnp.bfloat16)
    half = (rows, 2 * rows)
    inv[...] = (
        wave(
            lax.broadcasted_iota(jnp.int32, half, 1),
            lax.broadcasted_iota(jnp.int32, half, 0) + rows,
            rows,
        )
        / rows
    ).astype(jnp.bfloat16)

    def spectra(i, _):
        cols = pl.ds(pl.multiple_of(i * TILE, TILE), TILE)
        spectrum[:, cols] = dot(fwd[:, :rows], filt[:, cols])
        return 0

    lax.fori_loop(0, width // TILE, spectra, 0)

    total = squares[...]
    for k, copy in enumerate(sq_copies):
        copy.wait_recv()
        total = total + squares_in[k]
    mean_square = jnp.sum(total, axis=1, keepdims=True) / channels
    norm = 1.0 / jnp.sqrt(mean_square + 0.5)

    for c in range(CHUNKS):

        def short(i, _, c=c):
            cols = pl.ds(pl.multiple_of(c * wide + i * TILE, TILE), TILE)
            x = stream[:, cols].astype(jnp.float32) * gain_ref[:, cols] * norm
            ext[c, own, pl.ds(pl.multiple_of(i * TILE, TILE), TILE)] = (
                sinner[:, cols].astype(jnp.float32) * x
            ).astype(jnp.bfloat16)
            return 0

        lax.fori_loop(0, tiles, short, 0)

        @pl.when(has_next)
        def _(c=c):
            t_copies[c].start()

    for copy in key_loads[1:]:
        copy.wait()

    @pl.when(has_next)
    def _():
        for c in range(1, CHUNKS):
            k_copies[c].start()

    step = lax.broadcasted_iota(jnp.int32, (rows, TILE), 0).astype(jnp.float32)

    def powers(i, _):
        cols = pl.ds(pl.multiple_of(i * TILE, TILE), TILE)
        exponent = step * decay_ref[:, cols]
        power[:, cols] = jnp.exp(-exponent)
        inv_power[:, cols] = jnp.exp(exponent)
        return 0

    lax.fori_loop(0, width // TILE, powers, 0)
    for copy in loads[3:]:
        copy.wait()
    row = lax.broadcasted_iota(jnp.int32, (rows, 2 * rows), 0)
    column = lax.broadcasted_iota(jnp.int32, (rows, 2 * rows), 1)
    lower = (jnp.where(column >= rows, column - rows, column) <= row).astype(
        jnp.float32
    ).astype(jnp.bfloat16)

    def state_copy(c, target):
        return pltpu.make_async_remote_copy(
            src_ref=group_state.at[c],
            dst_ref=states.at[c, group],
            send_sem=e_send.at[c, target],
            recv_sem=e_recv.at[c, group],
            device_id={"seq": lax.rem(target * PAIR, n)},
            device_id_type=MESH,
        )

    p_copies = [
        pltpu.make_async_remote_copy(
            src_ref=own_state.at[c],
            dst_ref=pair_state.at[c],
            send_sem=p_send.at[c],
            recv_sem=p_recv.at[c],
            device_id={"seq": lax.rem(me + n - 1, n)},
            device_id_type=MESH,
        )
        for c in range(CHUNKS)
    ]
    q_copies = [
        pltpu.make_async_remote_copy(
            src_ref=next_state.at[c],
            dst_ref=carry_in.at[c],
            send_sem=q_send.at[c],
            recv_sem=q_recv.at[c],
            device_id={"seq": lax.rem(me + 1, n)},
            device_id_type=MESH,
        )
        for c in range(CHUNKS)
    ]

    for c in range(CHUNKS):

        @pl.when(has_prev)
        def _(c=c):
            t_copies[c].wait_recv()

        def mix(i, _, c=c):
            here = pl.ds(pl.multiple_of(i * TILE, TILE), TILE)
            cols = pl.ds(pl.multiple_of(c * wide + i * TILE, TILE), TILE)
            x = dot(fwd[...], ext[c, :, here])
            x_re, x_im = x[:rows], x[rows:]
            h_re, h_im = spectrum[:rows, cols], spectrum[rows:, cols]
            y = jnp.concatenate(
                [x_re * h_re - x_im * h_im, x_re * h_im + x_im * h_re], axis=0
            ).astype(jnp.bfloat16)
            conv = dot(inv[...], y)
            long_in = (
                linner[:, cols].astype(jnp.float32) * souter[:, cols].astype(jnp.float32) * conv
            ).astype(jnp.bfloat16)
            v = long_in.astype(jnp.float32) * inv_power[:, cols]
            high = v.astype(jnp.bfloat16)
            low = (v - high.astype(jnp.float32)).astype(jnp.bfloat16)
            sums = dot(lower, jnp.concatenate([high, low], axis=0))
            cum[:, cols] = sums
            own_state[c, :, here] = sums[rows - 1 :] * power[rows - 1 :, cols]
            return 0

        lax.fori_loop(0, tiles, mix, 0)

        @pl.when(follows)
        def _(c=c):
            p_copies[c].start()

        @pl.when(leads)
        def _(c=c):
            p_copies[c].wait_recv()
            rate = decay_ref[:, pl.ds(c * wide, wide)]
            group_state[c] = own_state[c] * jnp.exp(-rate * rows) + pair_state[c]

            def send_state(target, _, c=c):
                state_copy(c, target).start()
                return 0

            lax.fori_loop(group + 1, groups, send_state, 0)

    for c in range(CHUNKS):
        chunk = pl.ds(c * wide, wide)
        rate = decay_ref[:, chunk]

        @pl.when(leads)
        def _(c=c, rate=rate):
            over_group = jnp.exp(-rate * (rows * PAIR))

            def arrive(j, state):
                pltpu.make_async_remote_copy(
                    src_ref=group_state.at[c],
                    dst_ref=states.at[c, j],
                    send_sem=e_send.at[c, group],
                    recv_sem=e_recv.at[c, j],
                    device_id={"seq": j * PAIR},
                    device_id_type=MESH,
                ).wait_recv()
                return state * over_group + states[c, j]

            state = lax.fori_loop(0, group, arrive, jnp.zeros((1, wide), jnp.float32))
            next_state[c] = state * jnp.exp(-rate * rows) + own_state[c]
            q_copies[c].start()
            carry_in[c] = state

        @pl.when(follows)
        def _(c=c):
            q_copies[c].wait_recv()

        carried = carry_in[c]
        carried = carried * jnp.exp(-rate)
        z = 2.0 * rate
        scale = jnp.sqrt(jnp.tanh(0.5 * z) * (1.0 + jnp.exp(-z)))
        for i in range(tiles):
            here = pl.ds(i * TILE, TILE)
            cols = pl.ds(c * wide + i * TILE, TILE)
            part = slice(i * TILE, (i + 1) * TILE)
            conv = (cum[:, cols] + carried[:, part]) * power[:, cols]
            out = (
                louter[:, cols].astype(jnp.float32) * (conv * scale[:, part])
            ).astype(jnp.bfloat16)
            values[c, own, here] = out
            mixed[:, cols] = out

        @pl.when(has_next)
        def _(c=c):
            v_copies[c].start()

    valid = (column <= row + rows) & ((column >= rows) | has_prev)
    for c in range(CHUNKS):

        @pl.when(has_prev)
        def _(c=c):
            k_copies[c].wait_recv()

        def score(h, _, c=c):
            here = pl.ds(pl.multiple_of(h * HEAD_DIM, HEAD_DIM), HEAD_DIM)
            cols = pl.ds(pl.multiple_of(c * wide + h * HEAD_DIM, HEAD_DIM), HEAD_DIM)
            s = lax.dot_general(
                query[:, cols],
                keys[c, :, here],
                (((1,), (1,)), ((), ())),
                preferred_element_type=jnp.float32,
            ) * HEAD_DIM ** (-0.5)
            s = jnp.where(valid, s, -1e30)
            e = jnp.exp(s - jnp.max(s, axis=1, keepdims=True))
            e = e * (1.0 / jnp.sum(e, axis=1, keepdims=True))
            weights[c, h] = e.astype(jnp.bfloat16)
            return 0

        lax.fori_loop(0, heads, score, 0, unroll=2)

    for c in range(CHUNKS):

        @pl.when(has_prev)
        def _(c=c):
            v_copies[c].wait_recv()

        def gather(h, _, c=c):
            here = pl.ds(pl.multiple_of(h * HEAD_DIM, HEAD_DIM), HEAD_DIM)
            cols = pl.ds(pl.multiple_of(c * wide + h * HEAD_DIM, HEAD_DIM), HEAD_DIM)
            attended[:, cols] = dot(weights[c, h], values[c, :, here]).astype(jnp.bfloat16)
            return 0

        lax.fori_loop(0, heads, gather, 0, unroll=2)

    for copy in sq_copies:
        copy.wait_send()

    for c in range(CHUNKS):

        @pl.when(follows)
        def _(c=c):
            p_copies[c].wait_send()

        @pl.when(leads)
        def _(c=c):
            q_copies[c].wait_send()

            def sent(target, _):
                state_copy(c, target).wait_send()
                return 0

            lax.fori_loop(group + 1, groups, sent, 0)

    @pl.when(has_next)
    def _():
        for copy in k_copies + t_copies + v_copies:
            copy.wait_send()


def on_device(
    n,
    mp,
    stream,
    norm_gain,
    short_outer,
    short_inner,
    short_filter,
    long_outer,
    long_inner,
    long_decay,
    query_heads,
    key_heads,
):
    rows, width = stream.shape
    wide = width // CHUNKS
    bf16, f32 = jnp.bfloat16, jnp.float32
    anywhere = pl.BlockSpec(memory_space=pltpu.HBM)
    vmem = pl.BlockSpec(memory_space=pltpu.VMEM)
    dma = pltpu.SemaphoreType.DMA
    return pl.pallas_call(
        functools.partial(kernel, n, mp, float(width * mp)),
        out_shape=[jax.ShapeDtypeStruct((rows, width), bf16)] * 2,
        in_specs=[vmem] * 2 + [anywhere] * 8,
        out_specs=[vmem] * 2,
        scratch_shapes=[pltpu.VMEM((rows, width), bf16)] * 7
        + [
            pltpu.VMEM((2 * rows, 2 * rows), bf16),
            pltpu.VMEM((rows, 2 * rows), bf16),
        ]
        + [pltpu.VMEM((CHUNKS, 2 * rows, wide), bf16)] * 3
        + [pltpu.VMEM((rows, width), f32)] * 3
        + [
            pltpu.VMEM((2 * rows, width), f32),
            pltpu.VMEM((CHUNKS, wide // HEAD_DIM, rows, 2 * rows), bf16),
            pltpu.VMEM((rows, 128), f32),
            pltpu.VMEM((mp - 1, rows, 128), f32),
        ]
        + [pltpu.VMEM((CHUNKS, 1, wide), f32)] * 5
        + [
            pltpu.VMEM((CHUNKS, n // PAIR, 1, wide), f32),
            dma((7,)),
            dma((CHUNKS,)),
            dma((mp - 1,)),
            dma((mp - 1,)),
        ]
        + [dma((CHUNKS,))] * 10
        + [dma((CHUNKS, n // PAIR))] * 2,
        compiler_params=pltpu.CompilerParams(
            collective_id=0, has_side_effects=True, vmem_limit_bytes=51 * 1024 * 1024
        ),
    )(
        norm_gain.reshape(1, width),
        long_decay.reshape(1, width),
        stream,
        short_outer,
        short_inner,
        short_filter,
        long_outer,
        long_inner,
        query_heads,
        key_heads,
    )


def solution(mesh):
    return jax.shard_map(
        functools.partial(on_device, mesh.shape["seq"], mesh.shape["mp"]),
        mesh=mesh,
        in_specs=(
            P("seq", "mp"),
            P("mp"),
            P("seq", "mp"),
            P("seq", "mp"),
            P(None, "mp"),
            P("seq", "mp"),
            P("seq", "mp"),
            P("mp"),
            P("seq", "mp"),
            P("seq", "mp"),
        ),
        out_specs=(P("seq", "mp"), P("seq", "mp")),
        check_vma=False,
    )
```

```python
import functools

import jax
import jax.numpy as jnp
import numpy as np
from jax import lax
from jax.experimental import pallas as pl
from jax.experimental.pallas import tpu as pltpu
from jax.sharding import PartitionSpec as P

HEAD_DIM = 128
CHUNKS = 4
PAIR = 2
EARLY = 2
TILE = 256
MESH = pl.DeviceIdType.MESH


def wave(frequency, place, rows):
    shift = jnp.where(frequency >= rows, rows, 0)
    index = lax.rem((2 * lax.rem(frequency, rows) + 1) * place + shift, 4 * rows)
    return jnp.cos(index.astype(jnp.float32) * (np.pi / (2 * rows)))


def dot(a, b):
    return jnp.dot(a, b, preferred_element_type=jnp.float32)


def kernel(
    n,
    mp,
    channels,
    gain_hbm,
    decay_hbm,
    stream_hbm,
    souter_hbm,
    sinner_hbm,
    filt_hbm,
    louter_hbm,
    linner_hbm,
    query_hbm,
    key_hbm,
    mixed,
    attended,
    gain_ref,
    decay_ref,
    stream,
    souter,
    sinner,
    filt,
    louter,
    linner,
    query,
    fwd,
    inv,
    keys,
    values,
    ext,
    power,
    inv_power,
    cum,
    spectrum,
    weights,
    squares,
    squares_in,
    own_state,
    pair_state,
    group_state,
    next_state,
    carry_in,
    states,
    load_sem,
    key_sem,
    sq_send,
    sq_recv,
    k_send,
    k_recv,
    t_send,
    t_recv,
    v_send,
    v_recv,
    p_send,
    p_recv,
    q_send,
    q_recv,
    e_send,
    e_recv,
):
    me = lax.axis_index("seq")
    col = lax.axis_index("mp")
    rows, width = stream.shape
    wide = width // CHUNKS
    tiles = wide // TILE
    heads = wide // HEAD_DIM
    has_next = me < n - 1
    has_prev = me > 0
    groups = n // PAIR
    group = me // PAIR
    leads = lax.rem(me, PAIR) == 0
    follows = lax.rem(me, PAIR) != 0
    own = pl.ds(rows, rows)
    before = pl.ds(0, rows)

    barrier = pltpu.get_barrier_semaphore()

    def greet(target):
        pl.semaphore_signal(barrier, inc=1, device_id={"seq": target}, device_id_type=MESH)

    @pl.when(has_next)
    def _():
        greet(me + 1)

    @pl.when(has_prev)
    def _():
        greet(me - 1)

    @pl.when(leads)
    def _():
        def greet_leader(k, _):
            greet(lax.rem(me + PAIR * k, n))
            return 0

        lax.fori_loop(1, groups, greet_leader, 0)

    for k in range(1, mp):
        pl.semaphore_signal(
            barrier, inc=1, device_id={"mp": lax.rem(col + k, mp)}, device_id_type=MESH
        )

    pairs = [
        (stream_hbm, stream),
        (filt_hbm, filt),
        (sinner_hbm, sinner),
        (souter_hbm, souter),
        (linner_hbm, linner),
        (louter_hbm, louter),
        (query_hbm, query),
        (gain_hbm, gain_ref),
        (decay_hbm, decay_ref),
    ]
    loads = [pltpu.make_async_copy(s, d, load_sem.at[i]) for i, (s, d) in enumerate(pairs)]
    key_loads = [
        pltpu.make_async_copy(
            key_hbm.at[:, pl.ds(c * wide, wide)], keys.at[c, own], key_sem.at[c]
        )
        for c in range(CHUNKS)
    ]
    key_loads[0].start()
    loads[0].start()
    key_loads[1].start()
    for copy in loads[1:]:
        copy.start()
    for copy in key_loads[EARLY:]:
        copy.start()

    def to_next(buffer, c, send, recv):
        return pltpu.make_async_remote_copy(
            src_ref=buffer.at[c, own],
            dst_ref=buffer.at[c, before],
            send_sem=send.at[c],
            recv_sem=recv.at[c],
            device_id={"seq": lax.rem(me + 1, n)},
            device_id_type=MESH,
        )

    k_copies = [to_next(keys, c, k_send, k_recv) for c in range(CHUNKS)]
    t_copies = [to_next(ext, c, t_send, t_recv) for c in range(CHUNKS)]
    v_copies = [to_next(values, c, v_send, v_recv) for c in range(CHUNKS)]

    @pl.when(me == 0)
    def _():
        for c in range(CHUNKS):
            keys[c, :rows, :] = jnp.zeros((rows, wide), keys.dtype)
            values[c, :rows, :] = jnp.zeros((rows, wide), values.dtype)
            ext[c, :rows, :] = jnp.zeros((rows, wide), ext.dtype)

    greeted = has_next.astype(jnp.int32) + has_prev.astype(jnp.int32) + mp - 1
    pl.semaphore_wait(barrier, jnp.where(leads, greeted + groups - 1, greeted))
    for c in range(EARLY):
        key_loads[c].wait()

        @pl.when(has_next)
        def _(c=c):
            k_copies[c].start()

    loads[0].wait()

    def square(i, acc):
        x = stream[:, pl.ds(pl.multiple_of(i * 128, 128), 128)].astype(jnp.float32)
        return acc + x * x

    squares[...] = lax.fori_loop(
        0, width // 128, square, jnp.zeros((rows, 128), jnp.float32), unroll=4
    )
    sq_copies = [
        pltpu.make_async_remote_copy(
            src_ref=squares,
            dst_ref=squares_in.at[k - 1],
            send_sem=sq_send.at[k - 1],
            recv_sem=sq_recv.at[k - 1],
            device_id={"mp": lax.rem(col + k, mp)},
            device_id_type=MESH,
        )
        for k in range(1, mp)
    ]
    for copy in sq_copies:
        copy.start()
    for copy in loads[1:3] + loads[7:]:
        copy.wait()

    full = (2 * rows, 2 * rows)
    fwd[...] = wave(
        lax.broadcasted_iota(jnp.int32, full, 0), lax.broadcasted_iota(jnp.int32, full, 1), rows
    ).astype(jnp.bfloat16)
    half = (rows, 2 * rows)
    inv[...] = (
        wave(
            lax.broadcasted_iota(jnp.int32, half, 1),
            lax.broadcasted_iota(jnp.int32, half, 0) + rows,
            rows,
        )
        / rows
    ).astype(jnp.bfloat16)

    def spectra(i, _):
        cols = pl.ds(pl.multiple_of(i * TILE, TILE), TILE)
        spectrum[:, cols] = dot(fwd[:, :rows], filt[:, cols])
        return 0

    lax.fori_loop(0, width // TILE, spectra, 0)

    total = squares[...]
    for k, copy in enumerate(sq_copies):
        copy.wait_recv()
        total = total + squares_in[k]
    mean_square = jnp.sum(total, axis=1, keepdims=True) / channels
    norm = 1.0 / jnp.sqrt(mean_square + 0.5)

    for c in range(CHUNKS):

        def short(i, _, c=c):
            cols = pl.ds(pl.multiple_of(c * wide + i * TILE, TILE), TILE)
            x = stream[:, cols].astype(jnp.float32) * gain_ref[:, cols] * norm
            ext[c, own, pl.ds(pl.multiple_of(i * TILE, TILE), TILE)] = (
                sinner[:, cols].astype(jnp.float32) * x
            ).astype(jnp.bfloat16)
            return 0

        lax.fori_loop(0, tiles, short, 0)

        @pl.when(has_next)
        def _(c=c):
            t_copies[c].start()

    for copy in key_loads[EARLY:]:
        copy.wait()

    @pl.when(has_next)
    def _():
        for c in range(EARLY, CHUNKS):
            k_copies[c].start()

    step = lax.broadcasted_iota(jnp.int32, (rows, TILE), 0).astype(jnp.float32)

    def powers(i, _):
        cols = pl.ds(pl.multiple_of(i * TILE, TILE), TILE)
        exponent = step * decay_ref[:, cols]
        power[:, cols] = jnp.exp(-exponent)
        inv_power[:, cols] = jnp.exp(exponent)
        return 0

    lax.fori_loop(0, width // TILE, powers, 0)
    for copy in loads[3:7]:
        copy.wait()
    row = lax.broadcasted_iota(jnp.int32, (rows, 2 * rows), 0)
    column = lax.broadcasted_iota(jnp.int32, (rows, 2 * rows), 1)
    lower = (jnp.where(column >= rows, column - rows, column) <= row).astype(
        jnp.float32
    ).astype(jnp.bfloat16)

    def state_copy(c, target):
        return pltpu.make_async_remote_copy(
            src_ref=group_state.at[c],
            dst_ref=states.at[c, group],
            send_sem=e_send.at[c, target],
            recv_sem=e_recv.at[c, group],
            device_id={"seq": lax.rem(target * PAIR, n)},
            device_id_type=MESH,
        )

    p_copies = [
        pltpu.make_async_remote_copy(
            src_ref=own_state.at[c],
            dst_ref=pair_state.at[c],
            send_sem=p_send.at[c],
            recv_sem=p_recv.at[c],
            device_id={"seq": lax.rem(me + n - 1, n)},
            device_id_type=MESH,
        )
        for c in range(CHUNKS)
    ]
    q_copies = [
        pltpu.make_async_remote_copy(
            src_ref=next_state.at[c],
            dst_ref=carry_in.at[c],
            send_sem=q_send.at[c],
            recv_sem=q_recv.at[c],
            device_id={"seq": lax.rem(me + 1, n)},
            device_id_type=MESH,
        )
        for c in range(CHUNKS)
    ]

    for c in range(CHUNKS):

        @pl.when(has_prev)
        def _(c=c):
            t_copies[c].wait_recv()

        def mix(i, _, c=c):
            here = pl.ds(pl.multiple_of(i * TILE, TILE), TILE)
            cols = pl.ds(pl.multiple_of(c * wide + i * TILE, TILE), TILE)
            x = dot(fwd[...], ext[c, :, here])
            x_re, x_im = x[:rows], x[rows:]
            h_re, h_im = spectrum[:rows, cols], spectrum[rows:, cols]
            y = jnp.concatenate(
                [x_re * h_re - x_im * h_im, x_re * h_im + x_im * h_re], axis=0
            ).astype(jnp.bfloat16)
            conv = dot(inv[...], y)
            long_in = (
                linner[:, cols].astype(jnp.float32) * souter[:, cols].astype(jnp.float32) * conv
            ).astype(jnp.bfloat16)
            v = long_in.astype(jnp.float32) * inv_power[:, cols]
            high = v.astype(jnp.bfloat16)
            low = (v - high.astype(jnp.float32)).astype(jnp.bfloat16)
            sums = dot(lower, jnp.concatenate([high, low], axis=0))
            cum[:, cols] = sums
            own_state[c, :, here] = sums[rows - 1 :] * power[rows - 1 :, cols]
            return 0

        lax.fori_loop(0, tiles, mix, 0)

        @pl.when(follows)
        def _(c=c):
            p_copies[c].start()

        @pl.when(leads)
        def _(c=c):
            p_copies[c].wait_recv()
            rate = decay_ref[:, pl.ds(c * wide, wide)]
            group_state[c] = own_state[c] * jnp.exp(-rate * rows) + pair_state[c]

            def send_state(target, _, c=c):
                state_copy(c, target).start()
                return 0

            lax.fori_loop(group + 1, groups, send_state, 0)

    for c in range(CHUNKS):
        chunk = pl.ds(c * wide, wide)
        rate = decay_ref[:, chunk]

        @pl.when(leads)
        def _(c=c, rate=rate):
            over_group = jnp.exp(-rate * (rows * PAIR))

            def arrive(j, state):
                pltpu.make_async_remote_copy(
                    src_ref=group_state.at[c],
                    dst_ref=states.at[c, j],
                    send_sem=e_send.at[c, group],
                    recv_sem=e_recv.at[c, j],
                    device_id={"seq": j * PAIR},
                    device_id_type=MESH,
                ).wait_recv()
                return state * over_group + states[c, j]

            state = lax.fori_loop(0, group, arrive, jnp.zeros((1, wide), jnp.float32))
            next_state[c] = state * jnp.exp(-rate * rows) + own_state[c]
            q_copies[c].start()
            carry_in[c] = state

        @pl.when(follows)
        def _(c=c):
            q_copies[c].wait_recv()

        carried = carry_in[c]
        carried = carried * jnp.exp(-rate)
        z = 2.0 * rate
        scale = jnp.sqrt(jnp.tanh(0.5 * z) * (1.0 + jnp.exp(-z)))
        for i in range(tiles):
            here = pl.ds(i * TILE, TILE)
            cols = pl.ds(c * wide + i * TILE, TILE)
            part = slice(i * TILE, (i + 1) * TILE)
            conv = (cum[:, cols] + carried[:, part]) * power[:, cols]
            out = (
                louter[:, cols].astype(jnp.float32) * (conv * scale[:, part])
            ).astype(jnp.bfloat16)
            values[c, own, here] = out
            mixed[:, cols] = out

        @pl.when(has_next)
        def _(c=c):
            v_copies[c].start()

    valid = (column <= row + rows) & ((column >= rows) | has_prev)
    for c in range(CHUNKS):

        @pl.when(has_prev)
        def _(c=c):
            k_copies[c].wait_recv()

        def score(h, _, c=c):
            here = pl.ds(pl.multiple_of(h * HEAD_DIM, HEAD_DIM), HEAD_DIM)
            cols = pl.ds(pl.multiple_of(c * wide + h * HEAD_DIM, HEAD_DIM), HEAD_DIM)
            s = lax.dot_general(
                query[:, cols],
                keys[c, :, here],
                (((1,), (1,)), ((), ())),
                preferred_element_type=jnp.float32,
            ) * HEAD_DIM ** (-0.5)
            s = jnp.where(valid, s, -1e30)
            e = jnp.exp(s - jnp.max(s, axis=1, keepdims=True))
            e = e * (1.0 / jnp.sum(e, axis=1, keepdims=True))
            weights[c, h] = e.astype(jnp.bfloat16)
            return 0

        lax.fori_loop(0, heads, score, 0, unroll=2)

    for c in range(CHUNKS):

        @pl.when(has_prev)
        def _(c=c):
            v_copies[c].wait_recv()

        def gather(h, _, c=c):
            here = pl.ds(pl.multiple_of(h * HEAD_DIM, HEAD_DIM), HEAD_DIM)
            cols = pl.ds(pl.multiple_of(c * wide + h * HEAD_DIM, HEAD_DIM), HEAD_DIM)
            attended[:, cols] = dot(weights[c, h], values[c, :, here]).astype(jnp.bfloat16)
            return 0

        lax.fori_loop(0, heads, gather, 0, unroll=8)

    for copy in sq_copies:
        copy.wait_send()

    for c in range(CHUNKS):

        @pl.when(follows)
        def _(c=c):
            p_copies[c].wait_send()

        @pl.when(leads)
        def _(c=c):
            q_copies[c].wait_send()

            def sent(target, _):
                state_copy(c, target).wait_send()
                return 0

            lax.fori_loop(group + 1, groups, sent, 0)

    @pl.when(has_next)
    def _():
        for copy in k_copies + t_copies + v_copies:
            copy.wait_send()


def on_device(
    n,
    mp,
    stream,
    norm_gain,
    short_outer,
    short_inner,
    short_filter,
    long_outer,
    long_inner,
    long_decay,
    query_heads,
    key_heads,
):
    rows, width = stream.shape
    wide = width // CHUNKS
    bf16, f32 = jnp.bfloat16, jnp.float32
    anywhere = pl.BlockSpec(memory_space=pltpu.HBM)
    vmem = pl.BlockSpec(memory_space=pltpu.VMEM)
    dma = pltpu.SemaphoreType.DMA
    return pl.pallas_call(
        functools.partial(kernel, n, mp, float(width * mp)),
        out_shape=[jax.ShapeDtypeStruct((rows, width), bf16)] * 2,
        in_specs=[anywhere] * 10,
        out_specs=[vmem] * 2,
        scratch_shapes=[pltpu.VMEM((1, width), f32)] * 2
        + [pltpu.VMEM((rows, width), bf16)] * 7
        + [
            pltpu.VMEM((2 * rows, 2 * rows), bf16),
            pltpu.VMEM((rows, 2 * rows), bf16),
        ]
        + [pltpu.VMEM((CHUNKS, 2 * rows, wide), bf16)] * 3
        + [pltpu.VMEM((rows, width), f32)] * 3
        + [
            pltpu.VMEM((2 * rows, width), f32),
            pltpu.VMEM((CHUNKS, wide // HEAD_DIM, rows, 2 * rows), bf16),
            pltpu.VMEM((rows, 128), f32),
            pltpu.VMEM((mp - 1, rows, 128), f32),
        ]
        + [pltpu.VMEM((CHUNKS, 1, wide), f32)] * 5
        + [
            pltpu.VMEM((CHUNKS, n // PAIR, 1, wide), f32),
            dma((9,)),
            dma((CHUNKS,)),
            dma((mp - 1,)),
            dma((mp - 1,)),
        ]
        + [dma((CHUNKS,))] * 10
        + [dma((CHUNKS, n // PAIR))] * 2,
        compiler_params=pltpu.CompilerParams(
            collective_id=0, has_side_effects=True, vmem_limit_bytes=51 * 1024 * 1024
        ),
    )(
        norm_gain.reshape(1, width),
        long_decay.reshape(1, width),
        stream,
        short_outer,
        short_inner,
        short_filter,
        long_outer,
        long_inner,
        query_heads,
        key_heads,
    )


def solution(mesh):
    return jax.shard_map(
        functools.partial(on_device, mesh.shape["seq"], mesh.shape["mp"]),
        mesh=mesh,
        in_specs=(
            P("seq", "mp"),
            P("mp"),
            P("seq", "mp"),
            P("seq", "mp"),
            P(None, "mp"),
            P("seq", "mp"),
            P("seq", "mp"),
            P("mp"),
            P("seq", "mp"),
            P("seq", "mp"),
        ),
        out_specs=(P("seq", "mp"), P("seq", "mp")),
        check_vma=False,
    )
```

```python
import functools

import jax
import jax.numpy as jnp
import numpy as np
from jax import lax
from jax.experimental import pallas as pl
from jax.experimental.pallas import tpu as pltpu
from jax.sharding import PartitionSpec as P

HEAD_DIM = 128
CHUNKS = 8
PAIR = 2
EARLY = 3
TILE = 256
MESH = pl.DeviceIdType.MESH


def wave(frequency, place, rows):
    shift = jnp.where(frequency >= rows, rows, 0)
    index = lax.rem((2 * lax.rem(frequency, rows) + 1) * place + shift, 4 * rows)
    return jnp.cos(index.astype(jnp.float32) * (np.pi / (2 * rows)))


def dot(a, b):
    return jnp.dot(a, b, preferred_element_type=jnp.float32)


def kernel(
    n,
    mp,
    channels,
    gain_hbm,
    decay_hbm,
    stream_hbm,
    souter_hbm,
    sinner_hbm,
    filt_hbm,
    louter_hbm,
    linner_hbm,
    query_hbm,
    key_hbm,
    mixed,
    attended,
    gain_ref,
    decay_ref,
    stream,
    souter,
    sinner,
    filt,
    louter,
    linner,
    query,
    fwd,
    inv,
    keys,
    values,
    ext,
    power,
    inv_power,
    cum,
    spectrum,
    weights,
    squares,
    squares_in,
    own_state,
    pair_state,
    group_state,
    next_state,
    carry_in,
    states,
    load_sem,
    key_sem,
    sq_send,
    sq_recv,
    k_send,
    k_recv,
    t_send,
    t_recv,
    v_send,
    v_recv,
    p_send,
    p_recv,
    q_send,
    q_recv,
    e_send,
    e_recv,
):
    me = lax.axis_index("seq")
    col = lax.axis_index("mp")
    rows, width = stream.shape
    wide = width // CHUNKS
    tiles = wide // TILE
    heads = wide // HEAD_DIM
    has_next = me < n - 1
    has_prev = me > 0
    groups = n // PAIR
    group = me // PAIR
    leads = lax.rem(me, PAIR) == 0
    follows = lax.rem(me, PAIR) != 0
    own = pl.ds(rows, rows)
    before = pl.ds(0, rows)

    barrier = pltpu.get_barrier_semaphore()

    def greet(target):
        pl.semaphore_signal(barrier, inc=1, device_id={"seq": target}, device_id_type=MESH)

    @pl.when(has_next)
    def _():
        greet(me + 1)

    @pl.when(has_prev)
    def _():
        greet(me - 1)

    @pl.when(leads)
    def _():
        def greet_leader(k, _):
            greet(lax.rem(me + PAIR * k, n))
            return 0

        lax.fori_loop(1, groups, greet_leader, 0)

    for k in range(1, mp):
        pl.semaphore_signal(
            barrier, inc=1, device_id={"mp": lax.rem(col + k, mp)}, device_id_type=MESH
        )

    pairs = [
        (stream_hbm, stream),
        (filt_hbm, filt),
        (sinner_hbm, sinner),
        (souter_hbm, souter),
        (linner_hbm, linner),
        (louter_hbm, louter),
        (query_hbm, query),
        (gain_hbm, gain_ref),
        (decay_hbm, decay_ref),
    ]
    loads = [pltpu.make_async_copy(s, d, load_sem.at[i]) for i, (s, d) in enumerate(pairs)]
    key_loads = [
        pltpu.make_async_copy(
            key_hbm.at[:, pl.ds(c * wide, wide)], keys.at[c, own], key_sem.at[c]
        )
        for c in range(CHUNKS)
    ]
    for copy in key_loads[:EARLY]:
        copy.start()
    loads[0].start()
    for copy in loads[1:]:
        copy.start()
    for copy in key_loads[EARLY:]:
        copy.start()

    def to_next(buffer, c, send, recv):
        return pltpu.make_async_remote_copy(
            src_ref=buffer.at[c, own],
            dst_ref=buffer.at[c, before],
            send_sem=send.at[c],
            recv_sem=recv.at[c],
            device_id={"seq": lax.rem(me + 1, n)},
            device_id_type=MESH,
        )

    k_copies = [to_next(keys, c, k_send, k_recv) for c in range(CHUNKS)]
    t_copies = [to_next(ext, c, t_send, t_recv) for c in range(CHUNKS)]
    v_copies = [to_next(values, c, v_send, v_recv) for c in range(CHUNKS)]

    @pl.when(me == 0)
    def _():
        for c in range(CHUNKS):
            keys[c, :rows, :] = jnp.zeros((rows, wide), keys.dtype)
            values[c, :rows, :] = jnp.zeros((rows, wide), values.dtype)
            ext[c, :rows, :] = jnp.zeros((rows, wide), ext.dtype)

    greeted = has_next.astype(jnp.int32) + has_prev.astype(jnp.int32) + mp - 1
    pl.semaphore_wait(barrier, jnp.where(leads, greeted + groups - 1, greeted))
    for c in range(EARLY):
        key_loads[c].wait()

        @pl.when(has_next)
        def _(c=c):
            k_copies[c].start()

    loads[0].wait()

    def square(i, acc):
        x = stream[:, pl.ds(pl.multiple_of(i * 128, 128), 128)].astype(jnp.float32)
        return acc + x * x

    squares[...] = lax.fori_loop(
        0, width // 128, square, jnp.zeros((rows, 128), jnp.float32), unroll=4
    )
    sq_copies = [
        pltpu.make_async_remote_copy(
            src_ref=squares,
            dst_ref=squares_in.at[k - 1],
            send_sem=sq_send.at[k - 1],
            recv_sem=sq_recv.at[k - 1],
            device_id={"mp": lax.rem(col + k, mp)},
            device_id_type=MESH,
        )
        for k in range(1, mp)
    ]
    for copy in sq_copies:
        copy.start()
    for copy in loads[1:3] + loads[7:]:
        copy.wait()

    full = (2 * rows, 2 * rows)
    fwd[...] = wave(
        lax.broadcasted_iota(jnp.int32, full, 0), lax.broadcasted_iota(jnp.int32, full, 1), rows
    ).astype(jnp.bfloat16)
    half = (rows, 2 * rows)
    inv[...] = (
        wave(
            lax.broadcasted_iota(jnp.int32, half, 1),
            lax.broadcasted_iota(jnp.int32, half, 0) + rows,
            rows,
        )
        / rows
    ).astype(jnp.bfloat16)

    def spectra(i, _):
        cols = pl.ds(pl.multiple_of(i * TILE, TILE), TILE)
        spectrum[:, cols] = dot(fwd[:, :rows], filt[:, cols])
        return 0

    lax.fori_loop(0, width // TILE, spectra, 0)

    total = squares[...]
    for k, copy in enumerate(sq_copies):
        copy.wait_recv()
        total = total + squares_in[k]
    mean_square = jnp.sum(total, axis=1, keepdims=True) / channels
    norm = 1.0 / jnp.sqrt(mean_square + 0.5)

    for c in range(CHUNKS):

        def short(i, _, c=c):
            cols = pl.ds(pl.multiple_of(c * wide + i * TILE, TILE), TILE)
            x = stream[:, cols].astype(jnp.float32) * gain_ref[:, cols] * norm
            ext[c, own, pl.ds(pl.multiple_of(i * TILE, TILE), TILE)] = (
                sinner[:, cols].astype(jnp.float32) * x
            ).astype(jnp.bfloat16)
            return 0

        lax.fori_loop(0, tiles, short, 0)

        @pl.when(has_next)
        def _(c=c):
            t_copies[c].start()

    for copy in key_loads[EARLY:]:
        copy.wait()

    @pl.when(has_next)
    def _():
        for c in range(EARLY, CHUNKS):
            k_copies[c].start()

    step = lax.broadcasted_iota(jnp.int32, (rows, TILE), 0).astype(jnp.float32)

    def powers(i, _):
        cols = pl.ds(pl.multiple_of(i * TILE, TILE), TILE)
        exponent = step * decay_ref[:, cols]
        power[:, cols] = jnp.exp(-exponent)
        inv_power[:, cols] = jnp.exp(exponent)
        return 0

    lax.fori_loop(0, width // TILE, powers, 0)
    for copy in loads[3:7]:
        copy.wait()
    row = lax.broadcasted_iota(jnp.int32, (rows, 2 * rows), 0)
    column = lax.broadcasted_iota(jnp.int32, (rows, 2 * rows), 1)
    lower = (jnp.where(column >= rows, column - rows, column) <= row).astype(
        jnp.float32
    ).astype(jnp.bfloat16)

    def state_copy(c, target):
        return pltpu.make_async_remote_copy(
            src_ref=group_state.at[c],
            dst_ref=states.at[c, group],
            send_sem=e_send.at[c, target],
            recv_sem=e_recv.at[c, group],
            device_id={"seq": lax.rem(target * PAIR, n)},
            device_id_type=MESH,
        )

    p_copies = [
        pltpu.make_async_remote_copy(
            src_ref=own_state.at[c],
            dst_ref=pair_state.at[c],
            send_sem=p_send.at[c],
            recv_sem=p_recv.at[c],
            device_id={"seq": lax.rem(me + n - 1, n)},
            device_id_type=MESH,
        )
        for c in range(CHUNKS)
    ]
    q_copies = [
        pltpu.make_async_remote_copy(
            src_ref=next_state.at[c],
            dst_ref=carry_in.at[c],
            send_sem=q_send.at[c],
            recv_sem=q_recv.at[c],
            device_id={"seq": lax.rem(me + 1, n)},
            device_id_type=MESH,
        )
        for c in range(CHUNKS)
    ]

    for c in range(CHUNKS):

        @pl.when(has_prev)
        def _(c=c):
            t_copies[c].wait_recv()

        def mix(i, _, c=c):
            here = pl.ds(pl.multiple_of(i * TILE, TILE), TILE)
            cols = pl.ds(pl.multiple_of(c * wide + i * TILE, TILE), TILE)
            x = dot(fwd[...], ext[c, :, here])
            x_re, x_im = x[:rows], x[rows:]
            h_re, h_im = spectrum[:rows, cols], spectrum[rows:, cols]
            y = jnp.concatenate(
                [x_re * h_re - x_im * h_im, x_re * h_im + x_im * h_re], axis=0
            ).astype(jnp.bfloat16)
            conv = dot(inv[...], y)
            long_in = (
                linner[:, cols].astype(jnp.float32) * souter[:, cols].astype(jnp.float32) * conv
            ).astype(jnp.bfloat16)
            v = long_in.astype(jnp.float32) * inv_power[:, cols]
            high = v.astype(jnp.bfloat16)
            low = (v - high.astype(jnp.float32)).astype(jnp.bfloat16)
            sums = dot(lower, jnp.concatenate([high, low], axis=0))
            cum[:, cols] = sums
            own_state[c, :, here] = sums[rows - 1 :] * power[rows - 1 :, cols]
            return 0

        lax.fori_loop(0, tiles, mix, 0)

        @pl.when(follows)
        def _(c=c):
            p_copies[c].start()

        @pl.when(leads)
        def _(c=c):
            p_copies[c].wait_recv()
            rate = decay_ref[:, pl.ds(c * wide, wide)]
            group_state[c] = own_state[c] * jnp.exp(-rate * rows) + pair_state[c]

            def send_state(target, _, c=c):
                state_copy(c, target).start()
                return 0

            lax.fori_loop(group + 1, groups, send_state, 0)

    for c in range(CHUNKS):
        chunk = pl.ds(c * wide, wide)
        rate = decay_ref[:, chunk]

        @pl.when(leads)
        def _(c=c, rate=rate):
            over_group = jnp.exp(-rate * (rows * PAIR))

            def arrive(j, state):
                pltpu.make_async_remote_copy(
                    src_ref=group_state.at[c],
                    dst_ref=states.at[c, j],
                    send_sem=e_send.at[c, group],
                    recv_sem=e_recv.at[c, j],
                    device_id={"seq": j * PAIR},
                    device_id_type=MESH,
                ).wait_recv()
                return state * over_group + states[c, j]

            state = lax.fori_loop(0, group, arrive, jnp.zeros((1, wide), jnp.float32))
            next_state[c] = state * jnp.exp(-rate * rows) + own_state[c]
            q_copies[c].start()
            carry_in[c] = state

        @pl.when(follows)
        def _(c=c):
            q_copies[c].wait_recv()

        carried = carry_in[c]
        carried = carried * jnp.exp(-rate)
        z = 2.0 * rate
        scale = jnp.sqrt(jnp.tanh(0.5 * z) * (1.0 + jnp.exp(-z)))
        for i in range(tiles):
            here = pl.ds(i * TILE, TILE)
            cols = pl.ds(c * wide + i * TILE, TILE)
            part = slice(i * TILE, (i + 1) * TILE)
            conv = (cum[:, cols] + carried[:, part]) * power[:, cols]
            out = (
                louter[:, cols].astype(jnp.float32) * (conv * scale[:, part])
            ).astype(jnp.bfloat16)
            values[c, own, here] = out
            mixed[:, cols] = out

        @pl.when(has_next)
        def _(c=c):
            v_copies[c].start()

    valid = (column <= row + rows) & ((column >= rows) | has_prev)
    for c in range(CHUNKS):

        @pl.when(has_prev)
        def _(c=c):
            k_copies[c].wait_recv()

        def score(h, _, c=c):
            here = pl.ds(pl.multiple_of(h * HEAD_DIM, HEAD_DIM), HEAD_DIM)
            cols = pl.ds(pl.multiple_of(c * wide + h * HEAD_DIM, HEAD_DIM), HEAD_DIM)
            s = lax.dot_general(
                query[:, cols],
                keys[c, :, here],
                (((1,), (1,)), ((), ())),
                preferred_element_type=jnp.float32,
            ) * HEAD_DIM ** (-0.5)
            s = jnp.where(valid, s, -1e30)
            e = jnp.exp(s - jnp.max(s, axis=1, keepdims=True))
            e = e * (1.0 / jnp.sum(e, axis=1, keepdims=True))
            weights[c, h] = e.astype(jnp.bfloat16)
            return 0

        lax.fori_loop(0, heads, score, 0, unroll=2)

    for c in range(CHUNKS):

        @pl.when(has_prev)
        def _(c=c):
            v_copies[c].wait_recv()

        def gather(h, _, c=c):
            here = pl.ds(pl.multiple_of(h * HEAD_DIM, HEAD_DIM), HEAD_DIM)
            cols = pl.ds(pl.multiple_of(c * wide + h * HEAD_DIM, HEAD_DIM), HEAD_DIM)
            attended[:, cols] = dot(weights[c, h], values[c, :, here]).astype(jnp.bfloat16)
            return 0

        lax.fori_loop(0, heads, gather, 0, unroll=heads)

    for copy in sq_copies:
        copy.wait_send()

    for c in range(CHUNKS):

        @pl.when(follows)
        def _(c=c):
            p_copies[c].wait_send()

        @pl.when(leads)
        def _(c=c):
            q_copies[c].wait_send()

            def sent(target, _):
                state_copy(c, target).wait_send()
                return 0

            lax.fori_loop(group + 1, groups, sent, 0)

    @pl.when(has_next)
    def _():
        for copy in k_copies + t_copies + v_copies:
            copy.wait_send()


def on_device(
    n,
    mp,
    stream,
    norm_gain,
    short_outer,
    short_inner,
    short_filter,
    long_outer,
    long_inner,
    long_decay,
    query_heads,
    key_heads,
):
    rows, width = stream.shape
    wide = width // CHUNKS
    bf16, f32 = jnp.bfloat16, jnp.float32
    anywhere = pl.BlockSpec(memory_space=pltpu.HBM)
    vmem = pl.BlockSpec(memory_space=pltpu.VMEM)
    dma = pltpu.SemaphoreType.DMA
    return pl.pallas_call(
        functools.partial(kernel, n, mp, float(width * mp)),
        out_shape=[jax.ShapeDtypeStruct((rows, width), bf16)] * 2,
        in_specs=[anywhere] * 10,
        out_specs=[vmem] * 2,
        scratch_shapes=[pltpu.VMEM((1, width), f32)] * 2
        + [pltpu.VMEM((rows, width), bf16)] * 7
        + [
            pltpu.VMEM((2 * rows, 2 * rows), bf16),
            pltpu.VMEM((rows, 2 * rows), bf16),
        ]
        + [pltpu.VMEM((CHUNKS, 2 * rows, wide), bf16)] * 3
        + [pltpu.VMEM((rows, width), f32)] * 3
        + [
            pltpu.VMEM((2 * rows, width), f32),
            pltpu.VMEM((CHUNKS, wide // HEAD_DIM, rows, 2 * rows), bf16),
            pltpu.VMEM((rows, 128), f32),
            pltpu.VMEM((mp - 1, rows, 128), f32),
        ]
        + [pltpu.VMEM((CHUNKS, 1, wide), f32)] * 5
        + [
            pltpu.VMEM((CHUNKS, n // PAIR, 1, wide), f32),
            dma((9,)),
            dma((CHUNKS,)),
            dma((mp - 1,)),
            dma((mp - 1,)),
        ]
        + [dma((CHUNKS,))] * 10
        + [dma((CHUNKS, n // PAIR))] * 2,
        compiler_params=pltpu.CompilerParams(
            collective_id=0, has_side_effects=True, vmem_limit_bytes=51 * 1024 * 1024
        ),
    )(
        norm_gain.reshape(1, width),
        long_decay.reshape(1, width),
        stream,
        short_outer,
        short_inner,
        short_filter,
        long_outer,
        long_inner,
        query_heads,
        key_heads,
    )


def solution(mesh):
    return jax.shard_map(
        functools.partial(on_device, mesh.shape["seq"], mesh.shape["mp"]),
        mesh=mesh,
        in_specs=(
            P("seq", "mp"),
            P("mp"),
            P("seq", "mp"),
            P("seq", "mp"),
            P(None, "mp"),
            P("seq", "mp"),
            P("seq", "mp"),
            P("mp"),
            P("seq", "mp"),
            P("seq", "mp"),
        ),
        out_specs=(P("seq", "mp"), P("seq", "mp")),
        check_vma=False,
    )
```

```python
import functools

import jax
import jax.numpy as jnp
import numpy as np
from jax import lax
from jax.experimental import pallas as pl
from jax.experimental.pallas import tpu as pltpu
from jax.sharding import PartitionSpec as P

HEAD_DIM = 128
CHUNKS = 4
PAIR = 2
EARLY = 2
TILE = 256
MESH = pl.DeviceIdType.MESH


def wave(frequency, place, rows):
    shift = jnp.where(frequency >= rows, rows, 0)
    index = lax.rem((2 * lax.rem(frequency, rows) + 1) * place + shift, 4 * rows)
    return jnp.cos(index.astype(jnp.float32) * (np.pi / (2 * rows)))


def dot(a, b):
    return jnp.dot(a, b, preferred_element_type=jnp.float32)


def kernel(
    n,
    mp,
    channels,
    gain_hbm,
    decay_hbm,
    stream_hbm,
    souter_hbm,
    sinner_hbm,
    filt_hbm,
    louter_hbm,
    linner_hbm,
    query_hbm,
    key_hbm,
    mixed,
    attended,
    gain_ref,
    decay_ref,
    stream,
    souter,
    sinner,
    filt,
    louter,
    linner,
    query,
    fwd,
    inv,
    keys,
    values,
    ext,
    power,
    inv_power,
    cum,
    spectrum,
    weights,
    squares,
    squares_in,
    own_state,
    pair_state,
    group_state,
    next_state,
    carry_in,
    states,
    load_sem,
    key_sem,
    sq_send,
    sq_recv,
    k_send,
    k_recv,
    t_send,
    t_recv,
    v_send,
    v_recv,
    p_send,
    p_recv,
    q_send,
    q_recv,
    e_send,
    e_recv,
):
    me = lax.axis_index("seq")
    col = lax.axis_index("mp")
    rows, width = stream.shape
    wide = width // CHUNKS
    tiles = wide // TILE
    heads = wide // HEAD_DIM
    has_next = me < n - 1
    has_prev = me > 0
    groups = n // PAIR
    group = me // PAIR
    leads = lax.rem(me, PAIR) == 0
    follows = lax.rem(me, PAIR) != 0
    own = pl.ds(rows, rows)
    before = pl.ds(0, rows)

    barrier = pltpu.get_barrier_semaphore()

    def greet(target):
        pl.semaphore_signal(barrier, inc=1, device_id={"seq": target}, device_id_type=MESH)

    @pl.when(has_next)
    def _():
        greet(me + 1)

    @pl.when(has_prev)
    def _():
        greet(me - 1)

    @pl.when(leads)
    def _():
        def greet_leader(k, _):
            greet(lax.rem(me + PAIR * k, n))
            return 0

        lax.fori_loop(1, groups, greet_leader, 0)

    for k in range(1, mp):
        pl.semaphore_signal(
            barrier, inc=1, device_id={"mp": lax.rem(col + k, mp)}, device_id_type=MESH
        )

    pairs = [
        (stream_hbm, stream),
        (filt_hbm, filt),
        (sinner_hbm, sinner),
        (souter_hbm, souter),
        (linner_hbm, linner),
        (louter_hbm, louter),
        (query_hbm, query),
        (gain_hbm, gain_ref),
        (decay_hbm, decay_ref),
    ]
    loads = [pltpu.make_async_copy(s, d, load_sem.at[i]) for i, (s, d) in enumerate(pairs)]
    key_loads = [
        pltpu.make_async_copy(
            key_hbm.at[:, pl.ds(c * wide, wide)], keys.at[c, own], key_sem.at[c]
        )
        for c in range(CHUNKS)
    ]
    key_loads[0].start()
    loads[0].start()
    key_loads[1].start()
    for copy in loads[1:]:
        copy.start()
    for copy in key_loads[EARLY:]:
        copy.start()

    def to_next(buffer, c, send, recv):
        return pltpu.make_async_remote_copy(
            src_ref=buffer.at[c, own],
            dst_ref=buffer.at[c, before],
            send_sem=send.at[c],
            recv_sem=recv.at[c],
            device_id={"seq": lax.rem(me + 1, n)},
            device_id_type=MESH,
        )

    k_copies = [to_next(keys, c, k_send, k_recv) for c in range(CHUNKS)]
    t_copies = [to_next(ext, c, t_send, t_recv) for c in range(CHUNKS)]
    v_copies = [to_next(values, c, v_send, v_recv) for c in range(CHUNKS)]

    @pl.when(me == 0)
    def _():
        for c in range(CHUNKS):
            keys[c, :rows, :] = jnp.zeros((rows, wide), keys.dtype)
            values[c, :rows, :] = jnp.zeros((rows, wide), values.dtype)
            ext[c, :rows, :] = jnp.zeros((rows, wide), ext.dtype)

    greeted = has_next.astype(jnp.int32) + has_prev.astype(jnp.int32) + mp - 1
    pl.semaphore_wait(barrier, jnp.where(leads, greeted + groups - 1, greeted))
    for c in range(EARLY):
        key_loads[c].wait()

        @pl.when(has_next)
        def _(c=c):
            k_copies[c].start()

    loads[0].wait()

    def square(i, acc):
        x = stream[:, pl.ds(pl.multiple_of(i * 128, 128), 128)].astype(jnp.float32)
        return acc + x * x

    squares[...] = lax.fori_loop(
        0, width // 128, square, jnp.zeros((rows, 128), jnp.float32), unroll=4
    )
    sq_copies = [
        pltpu.make_async_remote_copy(
            src_ref=squares,
            dst_ref=squares_in.at[k - 1],
            send_sem=sq_send.at[k - 1],
            recv_sem=sq_recv.at[k - 1],
            device_id={"mp": lax.rem(col + k, mp)},
            device_id_type=MESH,
        )
        for k in range(1, mp)
    ]
    for copy in sq_copies:
        copy.start()
    for copy in loads[1:3] + loads[7:]:
        copy.wait()

    full = (2 * rows, 2 * rows)
    fwd[...] = wave(
        lax.broadcasted_iota(jnp.int32, full, 0), lax.broadcasted_iota(jnp.int32, full, 1), rows
    ).astype(jnp.bfloat16)
    half = (rows, 2 * rows)
    inv[...] = (
        wave(
            lax.broadcasted_iota(jnp.int32, half, 1),
            lax.broadcasted_iota(jnp.int32, half, 0) + rows,
            rows,
        )
        / rows
    ).astype(jnp.bfloat16)

    def spectra(i, _):
        cols = pl.ds(pl.multiple_of(i * TILE, TILE), TILE)
        spectrum[:, cols] = dot(fwd[:, :rows], filt[:, cols])
        return 0

    lax.fori_loop(0, width // TILE, spectra, 0)

    total = squares[...]
    for k, copy in enumerate(sq_copies):
        copy.wait_recv()
        total = total + squares_in[k]
    mean_square = jnp.sum(total, axis=1, keepdims=True) / channels
    norm = 1.0 / jnp.sqrt(mean_square + 0.5)

    for c in range(CHUNKS):

        def short(i, _, c=c):
            cols = pl.ds(pl.multiple_of(c * wide + i * TILE, TILE), TILE)
            x = stream[:, cols].astype(jnp.float32) * gain_ref[:, cols] * norm
            ext[c, own, pl.ds(pl.multiple_of(i * TILE, TILE), TILE)] = (
                sinner[:, cols].astype(jnp.float32) * x
            ).astype(jnp.bfloat16)
            return 0

        lax.fori_loop(0, tiles, short, 0)

        @pl.when(has_next)
        def _(c=c):
            t_copies[c].start()

    for copy in key_loads[EARLY:]:
        copy.wait()

    @pl.when(has_next)
    def _():
        for c in range(EARLY, CHUNKS):
            k_copies[c].start()

    step = lax.broadcasted_iota(jnp.int32, (rows, TILE), 0).astype(jnp.float32)

    def powers(i, _):
        cols = pl.ds(pl.multiple_of(i * TILE, TILE), TILE)
        exponent = step * decay_ref[:, cols]
        power[:, cols] = jnp.exp(-exponent)
        inv_power[:, cols] = jnp.exp(exponent)
        return 0

    lax.fori_loop(0, width // TILE, powers, 0)
    for copy in loads[3:7]:
        copy.wait()
    row = lax.broadcasted_iota(jnp.int32, (rows, 2 * rows), 0)
    column = lax.broadcasted_iota(jnp.int32, (rows, 2 * rows), 1)
    lower = (jnp.where(column >= rows, column - rows, column) <= row).astype(
        jnp.float32
    ).astype(jnp.bfloat16)

    valid = (column <= row + rows) & ((column >= rows) | has_prev)
    def attend(c):

        @pl.when(has_prev)
        def _():
            k_copies[c].wait_recv()

        def score(h, _):
            here = pl.ds(pl.multiple_of(h * HEAD_DIM, HEAD_DIM), HEAD_DIM)
            cols = pl.ds(pl.multiple_of(c * wide + h * HEAD_DIM, HEAD_DIM), HEAD_DIM)
            s = lax.dot_general(
                query[:, cols],
                keys[c, :, here],
                (((1,), (1,)), ((), ())),
                preferred_element_type=jnp.float32,
            ) * HEAD_DIM ** (-0.5)
            s = jnp.where(valid, s, -1e30)
            e = jnp.exp(s - jnp.max(s, axis=1, keepdims=True))
            e = e * (1.0 / jnp.sum(e, axis=1, keepdims=True))
            weights[c, h] = e.astype(jnp.bfloat16)
            return 0

        lax.fori_loop(0, heads, score, 0, unroll=2)

    for c in range(EARLY):
        attend(c)

    def state_copy(c, target):
        return pltpu.make_async_remote_copy(
            src_ref=group_state.at[c],
            dst_ref=states.at[c, group],
            send_sem=e_send.at[c, target],
            recv_sem=e_recv.at[c, group],
            device_id={"seq": lax.rem(target * PAIR, n)},
            device_id_type=MESH,
        )

    p_copies = [
        pltpu.make_async_remote_copy(
            src_ref=own_state.at[c],
            dst_ref=pair_state.at[c],
            send_sem=p_send.at[c],
            recv_sem=p_recv.at[c],
            device_id={"seq": lax.rem(me + n - 1, n)},
            device_id_type=MESH,
        )
        for c in range(CHUNKS)
    ]
    q_copies = [
        pltpu.make_async_remote_copy(
            src_ref=next_state.at[c],
            dst_ref=carry_in.at[c],
            send_sem=q_send.at[c],
            recv_sem=q_recv.at[c],
            device_id={"seq": lax.rem(me + 1, n)},
            device_id_type=MESH,
        )
        for c in range(CHUNKS)
    ]

    for c in range(CHUNKS):

        @pl.when(has_prev)
        def _(c=c):
            t_copies[c].wait_recv()

        def mix(i, _, c=c):
            here = pl.ds(pl.multiple_of(i * TILE, TILE), TILE)
            cols = pl.ds(pl.multiple_of(c * wide + i * TILE, TILE), TILE)
            x = dot(fwd[...], ext[c, :, here])
            x_re, x_im = x[:rows], x[rows:]
            h_re, h_im = spectrum[:rows, cols], spectrum[rows:, cols]
            y = jnp.concatenate(
                [x_re * h_re - x_im * h_im, x_re * h_im + x_im * h_re], axis=0
            ).astype(jnp.bfloat16)
            conv = dot(inv[...], y)
            long_in = (
                linner[:, cols].astype(jnp.float32) * souter[:, cols].astype(jnp.float32) * conv
            ).astype(jnp.bfloat16)
            v = long_in.astype(jnp.float32) * inv_power[:, cols]
            high = v.astype(jnp.bfloat16)
            low = (v - high.astype(jnp.float32)).astype(jnp.bfloat16)
            sums = dot(lower, jnp.concatenate([high, low], axis=0))
            cum[:, cols] = sums
            own_state[c, :, here] = sums[rows - 1 :] * power[rows - 1 :, cols]
            return 0

        lax.fori_loop(0, tiles, mix, 0)

        @pl.when(follows)
        def _(c=c):
            p_copies[c].start()

        @pl.when(leads)
        def _(c=c):
            p_copies[c].wait_recv()
            rate = decay_ref[:, pl.ds(c * wide, wide)]
            group_state[c] = own_state[c] * jnp.exp(-rate * rows) + pair_state[c]

            def send_state(target, _, c=c):
                state_copy(c, target).start()
                return 0

            lax.fori_loop(group + 1, groups, send_state, 0)

    for c in range(CHUNKS):
        chunk = pl.ds(c * wide, wide)
        rate = decay_ref[:, chunk]

        @pl.when(leads)
        def _(c=c, rate=rate):
            over_group = jnp.exp(-rate * (rows * PAIR))

            def arrive(j, state):
                pltpu.make_async_remote_copy(
                    src_ref=group_state.at[c],
                    dst_ref=states.at[c, j],
                    send_sem=e_send.at[c, group],
                    recv_sem=e_recv.at[c, j],
                    device_id={"seq": j * PAIR},
                    device_id_type=MESH,
                ).wait_recv()
                return state * over_group + states[c, j]

            state = lax.fori_loop(0, group, arrive, jnp.zeros((1, wide), jnp.float32))
            next_state[c] = state * jnp.exp(-rate * rows) + own_state[c]
            q_copies[c].start()
            carry_in[c] = state

        @pl.when(follows)
        def _(c=c):
            q_copies[c].wait_recv()

        carried = carry_in[c]
        carried = carried * jnp.exp(-rate)
        z = 2.0 * rate
        scale = jnp.sqrt(jnp.tanh(0.5 * z) * (1.0 + jnp.exp(-z)))
        for i in range(tiles):
            here = pl.ds(i * TILE, TILE)
            cols = pl.ds(c * wide + i * TILE, TILE)
            part = slice(i * TILE, (i + 1) * TILE)
            conv = (cum[:, cols] + carried[:, part]) * power[:, cols]
            out = (
                louter[:, cols].astype(jnp.float32) * (conv * scale[:, part])
            ).astype(jnp.bfloat16)
            values[c, own, here] = out
            mixed[:, cols] = out

        @pl.when(has_next)
        def _(c=c):
            v_copies[c].start()

    for c in range(EARLY, CHUNKS):
        attend(c)

    for c in range(CHUNKS):

        @pl.when(has_prev)
        def _(c=c):
            v_copies[c].wait_recv()

        def gather(h, _, c=c):
            here = pl.ds(pl.multiple_of(h * HEAD_DIM, HEAD_DIM), HEAD_DIM)
            cols = pl.ds(pl.multiple_of(c * wide + h * HEAD_DIM, HEAD_DIM), HEAD_DIM)
            attended[:, cols] = dot(weights[c, h], values[c, :, here]).astype(jnp.bfloat16)
            return 0

        lax.fori_loop(0, heads, gather, 0, unroll=8)

    for copy in sq_copies:
        copy.wait_send()

    for c in range(CHUNKS):

        @pl.when(follows)
        def _(c=c):
            p_copies[c].wait_send()

        @pl.when(leads)
        def _(c=c):
            q_copies[c].wait_send()

            def sent(target, _):
                state_copy(c, target).wait_send()
                return 0

            lax.fori_loop(group + 1, groups, sent, 0)

    @pl.when(has_next)
    def _():
        for copy in k_copies + t_copies + v_copies:
            copy.wait_send()


def on_device(
    n,
    mp,
    stream,
    norm_gain,
    short_outer,
    short_inner,
    short_filter,
    long_outer,
    long_inner,
    long_decay,
    query_heads,
    key_heads,
):
    rows, width = stream.shape
    wide = width // CHUNKS
    bf16, f32 = jnp.bfloat16, jnp.float32
    anywhere = pl.BlockSpec(memory_space=pltpu.HBM)
    vmem = pl.BlockSpec(memory_space=pltpu.VMEM)
    dma = pltpu.SemaphoreType.DMA
    return pl.pallas_call(
        functools.partial(kernel, n, mp, float(width * mp)),
        out_shape=[jax.ShapeDtypeStruct((rows, width), bf16)] * 2,
        in_specs=[anywhere] * 10,
        out_specs=[vmem] * 2,
        scratch_shapes=[pltpu.VMEM((1, width), f32)] * 2
        + [pltpu.VMEM((rows, width), bf16)] * 7
        + [
            pltpu.VMEM((2 * rows, 2 * rows), bf16),
            pltpu.VMEM((rows, 2 * rows), bf16),
        ]
        + [pltpu.VMEM((CHUNKS, 2 * rows, wide), bf16)] * 3
        + [pltpu.VMEM((rows, width), f32)] * 3
        + [
            pltpu.VMEM((2 * rows, width), f32),
            pltpu.VMEM((CHUNKS, wide // HEAD_DIM, rows, 2 * rows), bf16),
            pltpu.VMEM((rows, 128), f32),
            pltpu.VMEM((mp - 1, rows, 128), f32),
        ]
        + [pltpu.VMEM((CHUNKS, 1, wide), f32)] * 5
        + [
            pltpu.VMEM((CHUNKS, n // PAIR, 1, wide), f32),
            dma((9,)),
            dma((CHUNKS,)),
            dma((mp - 1,)),
            dma((mp - 1,)),
        ]
        + [dma((CHUNKS,))] * 10
        + [dma((CHUNKS, n // PAIR))] * 2,
        compiler_params=pltpu.CompilerParams(
            collective_id=0, has_side_effects=True, vmem_limit_bytes=51 * 1024 * 1024
        ),
    )(
        norm_gain.reshape(1, width),
        long_decay.reshape(1, width),
        stream,
        short_outer,
        short_inner,
        short_filter,
        long_outer,
        long_inner,
        query_heads,
        key_heads,
    )


def solution(mesh):
    return jax.shard_map(
        functools.partial(on_device, mesh.shape["seq"], mesh.shape["mp"]),
        mesh=mesh,
        in_specs=(
            P("seq", "mp"),
            P("mp"),
            P("seq", "mp"),
            P("seq", "mp"),
            P(None, "mp"),
            P("seq", "mp"),
            P("seq", "mp"),
            P("mp"),
            P("seq", "mp"),
            P("seq", "mp"),
        ),
        out_specs=(P("seq", "mp"), P("seq", "mp")),
        check_vma=False,
    )
```
